32 devices in a mesh: sector: 4 (over y, core), member: 8 (over z, x).
Axes of the slice: x: 2, y: 2, z: 4, core: 2. Of those that a mesh axis runs over, the one named last changes fastest.
Arguments:
- state: bfloat16 [16, 1024, 256], P('member', 'sector'), may hold values from -18 to 18
- window_mask: int32 [1024, 256], P('sector'), may hold values 0 or 1
- window_index: int32 [1024], replicated, may hold values from 0 to 7, never falling along the last dimension, each value on 1 to 256 neighbouring positions
- w_space_qkv: bfloat16 [256, 768], replicated, may hold values from -0.375 to 0.375
- w_space_out: bfloat16 [256, 256], replicated, may hold values from -0.375 to 0.375
- temp_space: float32 [8], replicated, may hold values from 0.5 to 64
- w_ens_qkv: bfloat16 [256, 768], replicated, may hold values from -0.375 to 0.375
- w_ens_out: bfloat16 [256, 256], replicated, may hold values from -0.375 to 0.375
- temp_ens: float32 [8], replicated, may hold values from 0.5 to 64
- w_in: bfloat16 [256, 1024], replicated, may hold values from -0.375 to 0.375
- w_out: bfloat16 [1024, 256], replicated, may hold values from -0.1875 to 0.1875
Outputs:
- out_state: bfloat16 [16, 1024, 256], P('member', 'sector')
The draws below stay inside these ranges and needn't reach their ends.
Inputs may be any that keep to these rules, and one draw needn't show every extreme that they name: `window_index`: window numbers never fall along the patches; a window spans 1 to 256 patches.
All inputs are finite; a program needn't handle non-finite values. No bound on the sum of `window_mask` on one device may be relied on, other than what follows from the above.
Results may differ from the reference program's by a relative error of at most 0.015.
The reference program's roundings to bfloat16 on the way count: a program that leaves them out, or rounds other values in their place, can miss the bound.
Values may be sent and summed in bfloat16 or wider, within the bound.
No kernel may reach another device: no remote copies, remote signals or barrier semaphores. Data moves between devices by JAX's collectives and lax.ppermute only.
A program may use at most 64 MiB of HBM per device.

```python
import math
import jax
import jax.numpy as jnp
import numpy as np
from jax import lax

D = 256
H = 8
FF = 1024
RAD = 128
TOK_DEV = 256
MEMBERS = 16
PATCHES = 1024


def draw_state(key, part):
    first, second = jax.random.split(jax.random.fold_in(key, 3))
    entries = jnp.clip(jax.random.normal(first, (MEMBERS, PATCHES, D), jnp.float32), -6.0, 6.0)
    scales = jnp.exp(jax.random.uniform(second, (MEMBERS, PATCHES, 1), jnp.float32, math.log(0.3), math.log(3.0)))
    return (entries * scales).astype(jnp.bfloat16)


def draw_sampling_heat(key, random_seed_offset):
    folded = jax.random.fold_in(key, random_seed_offset)
    lower, upper = (0.5, 2.0)
    return jnp.exp(jax.random.uniform(folded, (H,), jnp.float32, math.log(lower), math.log(upper)))


def draw_temp_space(key, part):
    return draw_sampling_heat(key, 11)


def draw_temp_ens(key, part):
    return draw_sampling_heat(key, 12)


def place_ends(array, own_key, smallest, high):
    longest = array.shape.index(max(array.shape))
    spots = []
    for shift in (0, 1):
        where = [jax.random.randint(jax.random.fold_in(own_key, axis), (), 0, length) for axis, length in enumerate(array.shape)]
        where[longest] = (where[longest] + shift) % array.shape[longest]
        spots.append(tuple(where))
    return array.at[spots[0]].set(smallest).at[spots[1]].set(high)


def split_up(count, total, bound, slope):
    loads = [(1 << 20) // math.isqrt(grade ** slope) + 1 for grade in range(2, count + 1)]
    surplus, given = total - bound - (count - 1), [1] * (count - 1)
    while surplus > 0:
        free = [i for i in range(count - 1) if given[i] < bound]
        pool, budget = sum([loads[i] for i in free]), surplus
        for i in free:
            more = min(bound - given[i], max(1, budget * loads[i] // pool), surplus)
            given[i] = given[i] + more
            surplus = surplus - more
    return np.array([bound] + given)


def uneven(key, number_of, total, limit, slope):
    if number_of == 2:
        one = jax.random.randint(key, (), max(1, total - limit), min(limit, total - 1) + 1)
        return jnp.stack([one, total - one])
    sizes = jnp.asarray(split_up(number_of, total, limit, slope), jnp.int32)
    pairs = (number_of - 1) // 2
    source_of, receiver = sizes[1:1 + 2 * pairs:2], sizes[2:2 + 2 * pairs:2]
    margin = jnp.minimum(source_of - 1, limit - receiver)
    shifted = jax.random.randint(jax.random.fold_in(key, 1), (pairs,), 0, 1 << 20) % (margin + 1)
    sizes = sizes.at[1:1 + 2 * pairs:2].set(source_of - shifted).at[2:2 + 2 * pairs:2].set(receiver + shifted)
    return sizes[jax.random.permutation(jax.random.fold_in(key, 2), number_of)]


def scatter_about(own_key, dims, spread, bound, kind=jnp.bfloat16):
    drawn = jax.random.normal(own_key, dims, jnp.float32) * spread
    return jnp.minimum(jnp.maximum(drawn, -bound), bound).astype(kind)


def setup_inputs(seed: int = 0) -> dict:
    key_of = jax.random.split(jax.random.key(seed), 12)
    state = draw_state(jax.random.fold_in(key_of[11], 71), 0)
    window_mask = place_ends((jax.random.randint(key_of[1], (PATCHES, 2 * RAD), 0, 2) < 1).astype(jnp.int32), jax.random.fold_in(key_of[1], 1), 0, 1)
    window_index = jnp.searchsorted(jnp.cumsum(uneven(key_of[2], PATCHES // RAD, PATCHES, 2 * RAD, 0)), jnp.arange(PATCHES), side="right").astype(jnp.int32)
    w_space_qkv = scatter_about(key_of[3], (D, 3 * D), D ** -0.5, 0.375)
    w_space_out = scatter_about(key_of[4], (D, D), D ** -0.5, 0.375)
    temp_space = draw_temp_space(jax.random.fold_in(key_of[11], 71), 0)
    w_ens_qkv = scatter_about(key_of[6], (D, 3 * D), D ** -0.5, 0.375)
    w_ens_out = scatter_about(key_of[7], (D, D), D ** -0.5, 0.375)
    temp_ens = draw_temp_ens(jax.random.fold_in(key_of[11], 71), 0)
    w_in = scatter_about(key_of[9], (D, FF), D ** -0.5, 0.375)
    w_out = scatter_about(key_of[10], (FF, D), FF ** -0.5, 0.1875)
    return {"state": state, "window_mask": window_mask, "window_index": window_index, "w_space_qkv": w_space_qkv, "w_space_out": w_space_out, "temp_space": temp_space, "w_ens_qkv": w_ens_qkv, "w_ens_out": w_ens_out, "temp_ens": temp_ens, "w_in": w_in, "w_out": w_out}


def rms_rows(values):
    squares = lax.optimization_barrier(jnp.mean(values * values, axis=-1, keepdims=True))
    return values * lax.rsqrt(squares + 1e-06)

def head_norm(values, total_heads):
    shaped = values.reshape(values.shape[:-1] + (total_heads, values.shape[-1] // total_heads))
    squares = lax.optimization_barrier(jnp.mean(shaped * shaped, axis=-1, keepdims=True))
    return (shaped * lax.rsqrt(squares + 0.1)).reshape(values.shape)

def skew_band(table, span_width):
    row_count, columns = table.shape
    padded = jnp.pad(table, ((0, 0), (0, span_width + 1 - columns)))
    return padded.reshape(-1)[:row_count * span_width].reshape(row_count, span_width)

def attend_window(queries, keys, values, query_window, key_window, mask_rows, logit_scale):
    span_width = keys.shape[1]
    banded = skew_band(mask_rows + 1, span_width)
    same_window = query_window[:, None] == key_window[None, :]
    allowed = (banded == 2) | (banded == 1) & same_window
    scores = jnp.einsum('mqhd,mkhd->mhqk', queries.astype(jnp.float32), keys.astype(jnp.float32))
    scores = scores * logit_scale[None, :, None, None]
    scores = jnp.where(allowed[None, None], scores, -1e+30)
    row_max = lax.optimization_barrier(jnp.max(scores, axis=-1, keepdims=True))
    exponent = jnp.exp(scores - row_max)
    weights = (exponent / lax.optimization_barrier(jnp.sum(exponent, axis=-1, keepdims=True))).astype(jnp.bfloat16)
    return jnp.einsum('mhqk,mkhd->mqhd', weights.astype(jnp.float32), values.astype(jnp.float32))

def member_attention_step(row_tile_size, query_key_value_weight, output_projection_weight, sampling_heat, total_heads):
    everyone, patch_count, features = row_tile_size.shape
    head_width = features // total_heads
    normed = rms_rows(row_tile_size.astype(jnp.float32)).astype(jnp.bfloat16)
    projected = jnp.dot(normed.reshape(-1, features), query_key_value_weight, preferred_element_type=jnp.float32)
    projected = projected.reshape(everyone, patch_count, 3 * features)
    shape_heads = (everyone, patch_count, total_heads, head_width)
    query_rows = head_norm(projected[..., :features], total_heads).astype(jnp.bfloat16).reshape(shape_heads)
    key_rows = head_norm(projected[..., features:2 * features], total_heads).astype(jnp.bfloat16).reshape(shape_heads)
    value_rows = projected[..., 2 * features:].astype(jnp.bfloat16).reshape(shape_heads)
    logit_scale = sampling_heat / math.sqrt(head_width)
    scores = jnp.einsum('mphd,nphd->phmn', query_rows.astype(jnp.float32), key_rows.astype(jnp.float32))
    scores = scores * logit_scale[None, :, None, None]
    row_max = lax.optimization_barrier(jnp.max(scores, axis=-1, keepdims=True))
    exponent = jnp.exp(scores - row_max)
    weights = (exponent / lax.optimization_barrier(jnp.sum(exponent, axis=-1, keepdims=True))).astype(jnp.bfloat16)
    mixed_heads = jnp.einsum('phmn,nphd->mphd', weights.astype(jnp.float32), value_rows.astype(jnp.float32))
    mixed_heads = mixed_heads.reshape(everyone * patch_count, features).astype(jnp.bfloat16)
    update = jnp.dot(mixed_heads, output_projection_weight, preferred_element_type=jnp.float32).reshape(row_tile_size.shape)
    return (row_tile_size.astype(jnp.float32) + update).astype(jnp.bfloat16)

def feed_forward(row_tile_size, w_in, w_out):
    features = row_tile_size.shape[-1]
    normed = rms_rows(row_tile_size.astype(jnp.float32)).astype(jnp.bfloat16).reshape(-1, features)
    hidden = jax.nn.gelu(jnp.dot(normed, w_in, preferred_element_type=jnp.float32)).astype(jnp.bfloat16)
    update = jnp.dot(hidden, w_out, preferred_element_type=jnp.float32).reshape(row_tile_size.shape)
    return (row_tile_size.astype(jnp.float32) + update).astype(jnp.bfloat16)

def reference(state, window_mask, window_index, w_space_qkv, w_space_out, temp_space, w_ens_qkv, w_ens_out, temp_ens, w_in, w_out):
    block_rows = min(TOK_DEV, 256)
    head_width = D // H
    cycle_index = jnp.concatenate([window_index[PATCHES - RAD:], window_index, window_index[:RAD]])
    logit_scale = temp_space / math.sqrt(head_width)
    offsets = jnp.arange(PATCHES // block_rows, dtype=jnp.int32) * block_rows

    def one_member(member_rows):
        normed = rms_rows(member_rows.astype(jnp.float32)).astype(jnp.bfloat16)
        projected = jnp.dot(normed, w_space_qkv, preferred_element_type=jnp.float32)
        query_rows = head_norm(projected[:, :D], H).astype(jnp.bfloat16).reshape(PATCHES, H, head_width)
        key_rows = head_norm(projected[:, D:2 * D], H).astype(jnp.bfloat16).reshape(PATCHES, H, head_width)
        value_rows = projected[:, 2 * D:].astype(jnp.bfloat16).reshape(PATCHES, H, head_width)
        key_cycle = jnp.concatenate([key_rows[PATCHES - RAD:], key_rows, key_rows[:RAD]])
        value_cycle = jnp.concatenate([value_rows[PATCHES - RAD:], value_rows, value_rows[:RAD]])

        def one_block(offset):
            queries = lax.dynamic_slice_in_dim(query_rows, offset, block_rows, 0)
            keys = lax.dynamic_slice_in_dim(key_cycle, offset, block_rows + 2 * RAD, 0)
            values = lax.dynamic_slice_in_dim(value_cycle, offset, block_rows + 2 * RAD, 0)
            query_window = lax.dynamic_slice_in_dim(window_index, offset, block_rows, 0)
            key_window = lax.dynamic_slice_in_dim(cycle_index, offset, block_rows + 2 * RAD, 0)
            mask_rows = lax.dynamic_slice_in_dim(window_mask, offset, block_rows, 0)
            return attend_window(queries[None], keys[None], values[None], query_window, key_window, mask_rows, logit_scale)[0]
        outputs = lax.map(one_block, offsets)
        mixed_heads = outputs.reshape(PATCHES, D).astype(jnp.bfloat16)
        update = jnp.dot(mixed_heads, w_space_out, preferred_element_type=jnp.float32)
        return (member_rows.astype(jnp.float32) + update).astype(jnp.bfloat16)
    state_b = lax.map(one_member, state)
    grouped = state_b.reshape(MEMBERS, PATCHES // block_rows, block_rows, D).transpose(1, 0, 2, 3)

    def one_group(row_tile_size):
        return feed_forward(member_attention_step(row_tile_size, w_ens_qkv, w_ens_out, temp_ens, H), w_in, w_out)
    outputs = lax.map(one_group, grouped)
    return outputs.transpose(1, 0, 2, 3).reshape(MEMBERS, PATCHES, D)
```

```python
import functools
import math

import jax
import jax.numpy as jnp
from jax import lax
from jax.experimental import pallas as pl
from jax.experimental.pallas import tpu as pltpu
from jax.sharding import PartitionSpec as P

F32 = jnp.float32
BF16 = jnp.bfloat16
LANES = 128
SUB = 8
LOG2E = math.log2(math.e)
OUTSIDE = -1e30


def dot(a, b):
    return lax.dot_general(a, b, (((1,), (0,)), ((), ())), preferred_element_type=F32)


def dot_lhs_t(a, b):
    return lax.dot_general(a, b, (((0,), (0,)), ((), ())), preferred_element_type=F32)


def dot_rhs_t(a, b):
    return lax.dot_general(a, b, (((1,), (1,)), ((), ())), preferred_element_type=F32)


def rms_rows(values):
    squares = jnp.mean(values * values, axis=-1, keepdims=True)
    return (values * lax.rsqrt(squares + 1e-06)).astype(BF16)


def head_norm_lanes(values, width):
    features = values.shape[-1]
    row = lax.broadcasted_iota(jnp.int32, (features, features), 0) // width
    col = lax.broadcasted_iota(jnp.int32, (features, features), 1) // width
    block = jnp.where(row == col, 1.0, 0.0).astype(BF16)
    squares = values * values
    high = squares.astype(BF16)
    low = (squares - high.astype(F32)).astype(BF16)
    means = (dot(high, block) + dot(low, block)) * (1.0 / width)
    return (values * lax.rsqrt(means + 0.1)).astype(BF16)


def head_norm_rows(values, width):
    features, count = values.shape
    shaped = values.reshape(features // width, width, count)
    means = jnp.mean(shaped * shaped, axis=1, keepdims=True)
    return (shaped * lax.rsqrt(means + 0.1)).reshape(features, count).astype(BF16)


def attend_rows(query_t, keys, value_t, bias, scales, width):
    features, count = query_t.shape
    span = keys.shape[0]
    per_tile = LANES // width
    ones = jnp.ones((16, span), BF16)
    mixed = []
    for first in range(0, features // width, 2):
        tile = first // per_tile
        tile_keys = keys[:, tile * LANES : (tile + 1) * LANES]
        padded = []
        for head in (first, first + 1):
            above = (head % per_tile) * width
            parts = []
            if above:
                parts.append(jnp.zeros((above, count), BF16))
            parts.append(query_t[head * width : (head + 1) * width])
            if LANES - above - width:
                parts.append(jnp.zeros((LANES - above - width, count), BF16))
            padded.append(jnp.concatenate(parts, axis=0))
        scores = dot(tile_keys, jnp.concatenate(padded, axis=1))
        powers = []
        for i in range(2):
            mine = scores[:, i * count : (i + 1) * count] + bias
            top = jnp.max(mine, axis=0, keepdims=True)
            powers.append(jnp.exp2((mine - top) * scales[first + i]).astype(BF16))
        left = jnp.concatenate([value_t[first * width : (first + 2) * width], ones], axis=0)
        both = dot(left, jnp.concatenate(powers, axis=1))
        for i in range(2):
            columns = slice(i * count, (i + 1) * count)
            total = both[2 * width : 2 * width + 1, columns]
            mixed.append(both[i * width : (i + 1) * width, columns] * (1.0 / total))
    return jnp.concatenate(mixed, axis=0)


def project_kernel(
    width, radius, state_ref, mask_ref, window_ref, weight_ref, key_ref, query_ref, value_ref, bias_ref
):
    members, tokens, features = state_ref.shape
    rows = members * tokens
    normed = rms_rows(state_ref[...].reshape(rows, features).astype(F32))
    key_ref[...] = head_norm_lanes(
        dot(normed, weight_ref[:, features : 2 * features]), width
    ).reshape(members, tokens, features)
    query_w = weight_ref[:, :features].T
    value_w = weight_ref[:, 2 * features :].T
    query_t = head_norm_rows(dot_rhs_t(query_w, normed), width)
    value_t = dot_rhs_t(value_w, normed).astype(BF16)
    for m in range(members):
        query_ref[m] = query_t[:, m * tokens : (m + 1) * tokens]
        value_ref[m] = value_t[:, m * tokens : (m + 1) * tokens]

    tiles = window_ref.shape[0]
    span = LANES + 2 * radius
    base = lax.axis_index("sector") * (tokens // LANES)
    for block in range(tokens // LANES):
        table = mask_ref[block * LANES : (block + 1) * LANES, :] + 1
        table = jnp.concatenate([table, jnp.zeros((LANES, span - 2 * radius), jnp.int32)], axis=1)
        banded = pltpu.roll(table, 0, 1, stride=1, stride_axis=0)
        own = jnp.broadcast_to(window_ref[pl.ds(base + block, 1), :], (LANES, LANES)).T
        for part in range(span // LANES):
            index = lax.rem(base + (tiles + block + part - radius // LANES), tiles)
            theirs = window_ref[pl.ds(index, 1), :]
            piece = banded[:, part * LANES : (part + 1) * LANES]
            allowed = (piece == 2) | ((piece == 1) & (own == theirs))
            bias = jnp.where(allowed, 0.0, OUTSIDE)
            bias_ref[block, part * LANES : (part + 1) * LANES, :] = bias.T


def window_kernel(
    width,
    share,
    state_ref,
    before_ref,
    after_ref,
    weight_ref,
    out_weight_ref,
    heat_ref,
    key_ref,
    query_ref,
    value_ref,
    bias_ref,
    parcel_ref,
):
    members, tokens, features = state_ref.shape
    radius = before_ref.shape[1]
    blocks = tokens // LANES
    span = bias_ref.shape[1]
    heads = features // width
    scales = [heat_ref[h] * (LOG2E / math.sqrt(width)) for h in range(heads)]
    edges = jnp.concatenate(
        [r[m] for m in range(members) for r in (before_ref, after_ref)], axis=0
    )
    normed = rms_rows(edges.astype(F32))
    edge_key = head_norm_lanes(dot(normed, weight_ref[:, features : 2 * features]), width)
    edge_value = dot_rhs_t(weight_ref[:, 2 * features :].T, normed).astype(BF16)
    results = []
    for m in range(members):
        at = 2 * m * radius
        keys = jnp.concatenate(
            [edge_key[at : at + radius], key_ref[m], edge_key[at + radius : at + 2 * radius]], axis=0
        )
        value_t = jnp.concatenate(
            [
                edge_value[:, at : at + radius],
                value_ref[m],
                edge_value[:, at + radius : at + 2 * radius],
            ],
            axis=1,
        )
        mixed = []
        for block in range(blocks):
            low = block * LANES
            mixed.append(
                attend_rows(
                    query_ref[m, :, low : low + LANES],
                    keys[low : low + span],
                    value_t[:, low : low + span],
                    bias_ref[block],
                    scales,
                    width,
                )
            )
        mixed = jnp.concatenate(mixed, axis=1).T.astype(BF16)
        results.append(state_ref[m].astype(F32) + dot(mixed, out_weight_ref[...]))
    parts = [r.reshape(tokens // SUB, 1, SUB, features) for r in results]
    packed = jnp.concatenate(parts, axis=1).reshape(members * tokens, features)
    parcel_ref[...] = packed.astype(BF16).reshape(parcel_ref.shape)


def member_kernel(
    width, parcel_ref, weight_ref, out_weight_ref, heat_ref, up_ref, down_ref, result_ref
):
    sources, groups, rows, features = parcel_ref.shape
    held = rows // SUB
    size = sources * rows
    heads = features // width
    scales = [heat_ref[h] * (LOG2E / math.sqrt(width)) for h in range(heads)]
    state = jnp.concatenate(
        [parcel_ref[:, g].reshape(size, features) for g in range(groups)], axis=0
    ).astype(F32)
    normed = rms_rows(state)
    keys = head_norm_lanes(dot(normed, weight_ref[:, features : 2 * features]), width)
    query_t = head_norm_rows(dot_rhs_t(weight_ref[:, :features].T, normed), width)
    value_t = dot_rhs_t(weight_ref[:, 2 * features :].T, normed).astype(BF16)
    key_patch = lax.rem(lax.broadcasted_iota(jnp.int32, (size, LANES), 0), SUB)
    query_patch = lax.rem(lax.broadcasted_iota(jnp.int32, (size, LANES), 1), SUB)
    bias = jnp.where(key_patch == query_patch, 0.0, OUTSIDE)
    mixed = []
    for g in range(groups):
        span = slice(g * size, (g + 1) * size)
        for low in range(g * size, (g + 1) * size, LANES):
            mixed.append(
                attend_rows(
                    query_t[:, low : low + LANES], keys[span], value_t[:, span], bias, scales, width
                )
            )
    mixed = jnp.concatenate(mixed, axis=1).T.astype(BF16)
    state = (state + dot(mixed, out_weight_ref[...])).astype(BF16).astype(F32)
    hidden = jax.nn.gelu(dot(rms_rows(state), up_ref[...])).astype(BF16)
    state = state + dot(hidden, down_ref[...])
    state = state.reshape(groups, sources, held, SUB, features)
    pieces = [
        state[g, s, m] for s in range(sources) for m in range(held) for g in range(groups)
    ]
    state = jnp.concatenate(pieces, axis=0).astype(BF16)
    result_ref[...] = state.reshape(result_ref.shape)


VMEM = pl.BlockSpec(memory_space=pltpu.VMEM)
SMEM = pl.BlockSpec(memory_space=pltpu.SMEM)


def on_device(
    state,
    window_mask,
    window_index,
    w_space_qkv,
    w_space_out,
    temp_space,
    w_ens_qkv,
    w_ens_out,
    temp_ens,
    w_in,
    w_out,
):
    members, tokens, features = state.shape
    width = features // temp_space.shape[0]
    radius = window_mask.shape[1] // 2
    sectors = lax.axis_size("sector")
    ring = [(i, (i + 1) % sectors) for i in range(sectors)]
    back = [(j, i) for i, j in ring]
    before = lax.ppermute(state[:, tokens - radius :], "sector", ring)
    after = lax.ppermute(state[:, :radius], "sector", back)
    blocks = tokens // LANES
    span = LANES + 2 * radius
    key, query, value, bias = pl.pallas_call(
        functools.partial(project_kernel, width, radius),
        out_shape=(
            jax.ShapeDtypeStruct((members, tokens, features), BF16),
            jax.ShapeDtypeStruct((members, features, tokens), BF16),
            jax.ShapeDtypeStruct((members, features, tokens), BF16),
            jax.ShapeDtypeStruct((blocks, span, LANES), F32),
        ),
        in_specs=[VMEM] * 4,
        out_specs=(VMEM,) * 4,
        name="project",
        cost_estimate=pl.CostEstimate(flops=10**9, transcendentals=0, bytes_accessed=10**6),
    )(state, window_mask, window_index.reshape(-1, LANES), w_space_qkv)

    group_size = lax.axis_size("member")
    share = tokens // group_size
    groups = share // SUB
    parcel = pl.pallas_call(
        functools.partial(window_kernel, width, share),
        out_shape=jax.ShapeDtypeStruct((group_size, groups, members * SUB, features), BF16),
        in_specs=[VMEM] * 5 + [SMEM] + [VMEM] * 4,
        out_specs=VMEM,
        name="window",
        cost_estimate=pl.CostEstimate(flops=10**9, transcendentals=0, bytes_accessed=10**6),
    )(state, before, after, w_space_qkv, w_space_out, temp_space, key, query, value, bias)
    parcel = lax.all_to_all(parcel, "member", split_axis=0, concat_axis=0, tiled=True)
    result = pl.pallas_call(
        functools.partial(member_kernel, width),
        out_shape=jax.ShapeDtypeStruct((group_size, members, share, features), BF16),
        in_specs=[VMEM] * 3 + [SMEM] + [VMEM] * 2,
        out_specs=VMEM,
        name="member",
        cost_estimate=pl.CostEstimate(flops=10**9, transcendentals=0, bytes_accessed=10**6),
    )(parcel, w_ens_qkv, w_ens_out, temp_ens, w_in, w_out)
    result = lax.all_to_all(result, "member", split_axis=0, concat_axis=0, tiled=True)
    return jnp.swapaxes(result, 0, 1).reshape(members, tokens, features)


def solution(mesh):
    return jax.shard_map(
        on_device,
        mesh=mesh,
        in_specs=(
            P("member", "sector", None),
            P("sector", None),
            P(),
            P(),
            P(),
            P(),
            P(),
            P(),
            P(),
            P(),
            P(),
        ),
        out_specs=P("member", "sector", None),
        check_vma=False,
    )
```
